32 devices in a mesh: cls: 4 (over z), site: 8 (over y, x, core).
Axes of the slice: x: 2, y: 2, z: 4, core: 2. Of those that a mesh axis runs over, the one named last changes fastest.
Arguments:
- tip_codes: int32 [1024, 8192], P('cls', 'site'), may hold values from 0 to 3
- counts: int32 [8192], P('site'), may hold values from 1 to 5
- children: int32 [1023, 2], replicated, may hold values from 0 to 2045, as said below
- lengths: float32 [4, 2046], replicated, may hold values from 0.01 to 1
- frequencies: float32 [4, 4], replicated, may hold values from 0.25 to 1.75
- weights: float32 [4], replicated, may hold values from 0.2 to 1
Outputs:
- site_loglik: float32 [4, 2048], P('cls', 'site')
- new_weights: float32 [4], P('cls')
- mean_loglik: float32 [], replicated
The draws below stay inside these ranges and needn't reach their ends.
Inputs may be any that keep to these rules, and one draw needn't show every extreme that they name: Row k lists the two children of internal node 1024 + k as node ids. Give the tips height 0 and the root height 10. The nodes of height h + 1 have exactly the nodes of height h as children, each once, and the root is node 2046. For every height h from 0 to 5, split the parents (height h + 1) and the children (height h) into 16 equal aligned blocks: the children of parent block j are child block j, so the tips j * 64 onward form clade j.
All inputs are finite; a program needn't handle non-finite values.
Results may differ from the reference program's by a relative error of at most 0.0003.
Values sent between devices are 32-bit elements; how exact they have to be, the bound alone decides.
A program may use at most 64 MiB of HBM per device.

```python
import math
import jax
import jax.numpy as jnp
from jax import lax

LEVELS = 10
TOP = 4
CLS = 4
SITE_DEV = 1024
TAXA = 1024
BRANCHES = 2046
SITES = 8192
N_SITE = 8


def draw_children(key, part):
    pieces = []
    for tree_level in range(LEVELS):
        level_below = TAXA >> tree_level
        if tree_level == 0:
            first_id = 0
        else:
            first_id = TAXA + TAXA - (TAXA >> tree_level - 1)
        if tree_level < LEVELS - TOP:
            blocks = 2 ** TOP
        else:
            blocks = 1
        block_size = level_below // blocks
        level_key = jax.random.fold_in(key, 17 + tree_level)
        block_keys = jax.random.split(level_key, blocks)
        shuffled = jax.vmap(lambda one_key: jax.random.permutation(one_key, block_size))(block_keys)
        shuffled = shuffled.astype(jnp.int32) + (jnp.arange(blocks, dtype=jnp.int32) * block_size)[:, None]
        pieces.append((shuffled.reshape(level_below // 2, 2) + first_id).astype(jnp.int32))
    return jnp.concatenate(pieces, axis=0)


def draw_counts(key, part):
    position = jnp.arange(SITES, dtype=jnp.int32)
    upper_end = 2 + 5 * position // SITES
    return jax.random.randint(jax.random.fold_in(key, 5), (SITES,), 1, upper_end, dtype=jnp.int32)


def with_ends(values, own_key, low, high):
    dims = values.shape
    spot = [jax.random.randint(jax.random.fold_in(own_key, axis), (), 0, dims[axis]) for axis in range(len(dims))]
    values = values.at[tuple(spot)].set(low)
    longest = dims.index(max(dims))
    spot[longest] = (spot[longest] + 1) % dims[longest]
    return values.at[tuple(spot)].set(high)


def setup_inputs(seed: int = 0) -> dict:
    keys = jax.random.split(jax.random.key(seed), 7)
    return {
        "tip_codes": with_ends(jax.random.randint(keys[0], (TAXA, SITES), 0, 4), jax.random.fold_in(keys[0], 1), 0, 3).astype(jnp.int32),
        "counts": draw_counts(jax.random.fold_in(keys[6], 71), 0),
        "children": draw_children(jax.random.fold_in(keys[6], 71), 0),
        "lengths": jnp.clip(jnp.exp(jax.random.uniform(keys[3], (CLS, BRANCHES), jnp.float32, math.log(0.01), math.log(1.0))), 0.01, 1.0),
        "frequencies": jnp.clip(1.0 + 0.15 * jax.random.normal(keys[4], (CLS, 4), jnp.float32), 0.25, 1.75),
        "weights": jnp.clip(jnp.exp(jax.random.uniform(keys[5], (CLS,), jnp.float32, math.log(0.2), math.log(1.0))), 0.2, 1.0),
    }


def transit(values, decays, stationary):
    average = jnp.sum(stationary[None, :, None] * values, axis=1, keepdims=True)
    return decays[:, None, None] * values + (1.0 - decays)[:, None, None] * average


def from_codes(codes, decays, stationary):
    states = jnp.arange(4, dtype=jnp.int32)
    onehot = (codes[:, None, :] == states[None, :, None]).astype(jnp.float32)
    return transit(onehot, decays, stationary)


def join_pair(left_part, right_part, scale_sum):
    parent = left_part * right_part
    largest = jnp.max(parent, axis=1, keepdims=True)
    return parent / largest, scale_sum + jnp.log(largest)


def class_loglik(tip_block, children, length_row, stationary):
    rate_scale = 1.0 / (1.0 - jnp.sum(stationary * stationary))
    values = None
    scales = None
    for tree_level in range(LEVELS):
        node_count = TAXA >> (tree_level + 1)
        offset = TAXA - (TAXA >> tree_level)
        child_ids = children[offset:offset + node_count]
        left_ids = child_ids[:, 0]
        right_ids = child_ids[:, 1]
        left_decay = jnp.exp(-rate_scale * length_row[left_ids])
        right_decay = jnp.exp(-rate_scale * length_row[right_ids])
        if tree_level == 0:
            left_part = from_codes(tip_block[left_ids], left_decay, stationary)
            right_part = from_codes(tip_block[right_ids], right_decay, stationary)
            scale_sum = jnp.zeros((node_count, 1, tip_block.shape[1]), jnp.float32)
        else:
            anchor = TAXA + TAXA - (TAXA >> (tree_level - 1))
            left_rows = (left_ids - anchor).astype(jnp.int32)
            right_rows = (right_ids - anchor).astype(jnp.int32)
            left_part = transit(values[left_rows], left_decay, stationary)
            right_part = transit(values[right_rows], right_decay, stationary)
            scale_sum = scales[left_rows] + scales[right_rows]
        values, scales = join_pair(left_part, right_part, scale_sum)
    return scales[0, 0] + jnp.log(jnp.sum(stationary[:, None] * values[0], axis=0))


def reference(tip_codes, counts, children, lengths, frequencies, weights):
    stationary = frequencies / jnp.sum(frequencies, axis=1, keepdims=True)
    log_weight = jnp.log(weights / jnp.sum(weights))
    block_count = SITES // SITE_DEV
    tip_blocks = tip_codes.reshape(TAXA, block_count, SITE_DEV).transpose(1, 0, 2)

    def one_block(tip_block):
        return jnp.stack([class_loglik(tip_block, children, lengths[class_no], stationary[class_no]) for class_no in range(CLS)])

    per_class = lax.map(one_block, tip_blocks)
    per_class = per_class.transpose(1, 0, 2).reshape(CLS, SITES)
    shifted = per_class + log_weight[:, None]
    largest = jnp.max(shifted, axis=0)
    site_total = largest + jnp.log(jnp.sum(jnp.exp(shifted - largest[None, :]), axis=0))
    posterior = jnp.exp(shifted - site_total[None, :])
    pattern_weight = counts.astype(jnp.float32)
    class_mass = jnp.sum(pattern_weight[None, :] * posterior, axis=1)
    all_count = jnp.sum(pattern_weight)
    new_weights = class_mass / all_count
    mean_loglik = jnp.sum(pattern_weight * site_total) / (all_count * TAXA)
    per_taxon = (site_total / TAXA).reshape(N_SITE, CLS, SITE_DEV // CLS).transpose(1, 0, 2).reshape(CLS, SITES // CLS)
    return per_taxon, new_weights, mean_loglik
```

```python
import functools

import jax
import jax.numpy as jnp
from jax import lax
from jax.experimental import pallas as pl
from jax.experimental.pallas import tpu as pltpu
from jax.sharding import PartitionSpec as P

LEVELS = 10
TOP = 4
LANES = 128
MESH = pl.DeviceIdType.MESH


def level_base(taxa, h):
    return 0 if h == 0 else 2 * taxa - (taxa >> (h - 1))


def kernel(
    groups,
    site_devices,
    codes_hbm,
    counts_ref,
    kids_ref,
    kids_smem,
    lengths_ref,
    freq_ref,
    weights_ref,
    result,
    codes,
    picked,
    table,
    grow,
    grow_up,
    stat,
    sent,
    got,
    upper,
    part,
    part_got,
    code_sem,
    send_sem,
    recv_sem,
    part_send,
    part_recv,
):
    g = lax.axis_index("cls")
    me = lax.axis_index("site")
    local, sites = codes_hbm.shape
    taxa = local * groups
    classes, branches = lengths_ref.shape
    quarter = sites // groups
    halves = quarter // LANES
    low = LEVELS - TOP
    clades = local >> low
    rows = halves * classes
    f32 = jnp.float32
    bf16 = jnp.bfloat16

    fetch = pltpu.make_async_copy(codes_hbm, codes, code_sem)
    fetch.start()

    barrier = pltpu.get_barrier_semaphore()
    others = [(a, b) for a in range(groups) for b in range(site_devices) if a or b]
    for a, b in others:
        pl.semaphore_signal(
            barrier,
            inc=1,
            device_id={"cls": lax.rem(g + a, groups), "site": lax.rem(me + b, site_devices)},
            device_id_type=MESH,
        )

    freq = freq_ref[...]
    pi = freq / jnp.sum(freq, axis=1, keepdims=True)
    beta = 1.0 / (1.0 - jnp.sum(pi * pi, axis=1, keepdims=True))
    lengths = lengths_ref[...]
    r = jnp.exp(beta * lengths) - 1.0
    drift = beta * jnp.sum(lengths, axis=1, keepdims=True)

    table[...] = jnp.zeros_like(table)
    hi = r.astype(bf16).astype(f32)
    rest = r - hi
    mid = rest.astype(bf16).astype(f32)
    table[0:classes, 0:branches] = hi
    table[classes : 2 * classes, 0:branches] = mid
    table[2 * classes : 3 * classes, 0:branches] = rest - mid
    kids = kids_ref[...]
    table[12:14, taxa : taxa + kids.shape[1]] = (kids >> 8).astype(f32)
    table[14:16, taxa : taxa + kids.shape[1]] = (kids & 255).astype(f32)

    pi8 = jnp.concatenate([pi] * halves, axis=0)
    for c in range(classes):
        for i in range(4):
            wide = jnp.broadcast_to(pi[:, i : i + 1], (classes, LANES))
            stat[c, i] = jnp.broadcast_to(wide[c : c + 1], (8, LANES))
    first_up = level_base(taxa, low)
    window = first_up // LANES * LANES
    r8 = jnp.concatenate([r[:, window:branches]] * halves, axis=0)
    for j in range(branches - first_up):
        at = first_up - window + j
        grow_up[j] = jnp.broadcast_to(r8[:, at : at + 1], (rows, LANES))

    q = lax.broadcasted_iota(jnp.int32, (1, local), 1)
    ancestor = (first_up + g * clades + (q & (clades - 1))).astype(f32)
    offset = {}
    total_rows = 0
    for h in range(low):
        offset[h] = total_rows
        total_rows += local >> h
    for h in range(low, -1, -1):
        count = local >> h
        base = level_base(taxa, h)
        if count % LANES == 0:
            start = pl.multiple_of(base + g * count, LANES)
            width = count
        else:
            start = base // LANES * LANES
            end = base + (taxa >> h)
            width = -(-end // LANES) * LANES - start
        ids = lax.broadcasted_iota(jnp.int32, (width, local), 0) + start
        onehot = (ids.astype(f32) == ancestor).astype(f32).astype(bf16)
        part_table = table[:, pl.ds(start, width)].astype(bf16)
        out = jnp.dot(part_table, onehot, preferred_element_type=f32)
        if h < low:
            r_row = out[0:classes] + out[classes : 2 * classes] + out[2 * classes : 3 * classes]
            r_col = jnp.concatenate([r_row, r_row], axis=0).T
            for c in range(classes):
                grow[c, offset[h] : offset[h] + count, :] = jnp.broadcast_to(
                    r_col[:count, c : c + 1], (count, LANES)
                )
        if h > 0:
            left = out[12:13] * 256.0 + out[14:15]
            right = out[13:14] * 256.0 + out[15:16]
            ancestor = jnp.where((q & count) != 0, right, left)
    tip_col = jnp.broadcast_to(ancestor, (8, local)).T[:, 0:1]
    tip_ids = (lax.broadcasted_iota(jnp.int32, (local, local), 1) + g * local).astype(f32)
    order = (tip_ids == tip_col).astype(f32).astype(bf16)

    fetch.wait()

    def quarter_of(k, dest):
        block = lax.rem(g + k, groups)
        for half in range(halves):
            lanes = pl.ds(pl.multiple_of(block * quarter + half * LANES, LANES), LANES)
            picked[half] = jnp.dot(
                order, codes[:, lanes].astype(f32).astype(bf16), preferred_element_type=f32
            )

        def one(step, carry):
            half = step // (classes // 2)
            pair = lax.rem(step, classes // 2) * 2
            both = (0, 1)
            pis = [[stat[pair + b, i] for i in range(4)] for b in both]

            def factor(b, h, n):
                return grow[pair + b, offset[h] + 8 * n : offset[h] + 8 * n + 8, :]

            def tip(n):
                code = picked[half, 8 * n : 8 * n + 8, :]
                marks = [code == float(i) for i in range(4)]
                result = []
                for b in both:
                    own = jnp.where(marks[2], pis[b][2], pis[b][3])
                    own = jnp.where(marks[0], pis[b][0], jnp.where(marks[1], pis[b][1], own))
                    off = factor(b, 0, n) * own
                    on = off + 1.0
                    result.append([jnp.where(mark, on, off) for mark in marks])
                return result

            def spread(b, values, scale):
                mean = (values[0] * pis[b][0] + values[1] * pis[b][1]) + (
                    values[2] * pis[b][2] + values[3] * pis[b][3]
                )
                move = scale * mean
                return [value + move for value in values]

            logs = ([], [])

            def node(h, n):
                if h == 0:
                    return tip(n)
                gap = (local >> h) // 8
                left = node(h - 1, n)
                right = node(h - 1, n + gap)
                result = []
                for b in both:
                    one_left, one_right = left[b], right[b]
                    if h > 1:
                        one_left = spread(b, one_left, factor(b, h - 1, n))
                        one_right = spread(b, one_right, factor(b, h - 1, n + gap))
                    values = [x * y for x, y in zip(one_left, one_right)]
                    if h == 3:
                        largest = jnp.maximum(
                            jnp.maximum(values[0], values[1]), jnp.maximum(values[2], values[3])
                        )
                        scale = pl.reciprocal(largest, approx=True)
                        logs[b].append(jnp.log(scale))
                        values = [value * scale for value in values]
                    result.append(values)
                return result

            ends = node(low - 1, 0)
            for b in both:
                row = pl.ds(half * classes + pair + b, 1)
                values = spread(b, ends[b], factor(b, low - 1, 0))
                values = [value[0:clades] * value[clades : 2 * clades] for value in values]
                log_sum = jnp.sum(sum(logs[b][1:], logs[b][0]), axis=0, keepdims=True)
                log_sum = jnp.sum(jnp.log(values[3]), axis=0, keepdims=True) - log_sum
                inverse = 1.0 / values[3]
                for i in range(3):
                    ratio = values[i] * inverse
                    for j in range(clades):
                        dest[j * 3 + i, row, :] = ratio[j : j + 1]
                dest[clades * 3, row, :] = log_sum
            return carry

        lax.fori_loop(0, rows // 2, one, 0)

    copies = []
    for place, k in enumerate([2, 1, 3] if groups == 4 else range(1, groups)):
        quarter_of(k, sent.at[k])
        if place == 0:
            pl.semaphore_wait(barrier, len(others))
        copy = pltpu.make_async_remote_copy(
            src_ref=sent.at[k],
            dst_ref=got.at[k],
            send_sem=send_sem.at[k],
            recv_sem=recv_sem.at[k],
            device_id={"cls": lax.rem(g + k, groups)},
            device_id_type=MESH,
        )
        copy.start()
        copies.append(copy)
    quarter_of(0, got.at[0])
    for copy in copies:
        copy.wait()

    pis8 = [jnp.broadcast_to(pi8[:, i : i + 1], (rows, LANES)) for i in range(4)]
    scales = got[0, clades * 3]
    for k in range(1, groups):
        scales = scales + got[k, clades * 3]

    def child(tree_level, ident):
        if tree_level == low:
            clade = jnp.clip(ident - first_up, 0, 2**TOP - 1)
            k = lax.rem(g + groups - clade // clades, groups)
            row = lax.rem(clade, clades) * 3
            values = [got[k, row + i] for i in range(3)] + [jnp.ones((rows, LANES), f32)]
        else:
            at = jnp.clip(ident - level_base(taxa, low + 1), 0, 2**TOP - 1)
            values = [upper[at, i] for i in range(4)]
        mean = (values[0] * pis8[0] + values[1] * pis8[1]) + (
            values[2] * pis8[2] + values[3] * pis8[3]
        )
        move = grow_up[jnp.clip(ident - first_up, 0, branches - first_up - 1)] * mean
        return [value + move for value in values]

    place = 0
    for tree_level in range(low, LEVELS):
        count = taxa >> (tree_level + 1)
        first = taxa - (taxa >> tree_level)
        for n in range(count):
            left = child(tree_level, kids_smem[0, first + n])
            right = child(tree_level, kids_smem[1, first + n])
            values = [a * b for a, b in zip(left, right)]
            largest = jnp.maximum(
                jnp.maximum(values[0], values[1]), jnp.maximum(values[2], values[3])
            )
            scale = pl.reciprocal(largest, approx=True)
            scales = scales - jnp.log(scale)
            values = [value * scale for value in values]
            if tree_level < LEVELS - 1:
                for i in range(4):
                    upper[place, i] = values[i]
                place += 1
    end = (values[0] * pis8[0] + values[1] * pis8[1]) + (
        values[2] * pis8[2] + values[3] * pis8[3]
    )
    spot = lax.broadcasted_iota(jnp.int32, (classes, classes), 0)
    spot = spot == lax.broadcasted_iota(jnp.int32, (classes, classes), 1)
    weights = jnp.sum(jnp.where(spot, weights_ref[...], 0.0), axis=1, keepdims=True)
    log_weight = jnp.log(weights / jnp.sum(weights, axis=0, keepdims=True))
    bias = jnp.concatenate([log_weight - drift] * halves, axis=0)
    shifted = scales + jnp.log(end) + bias

    mass = jnp.zeros((classes, LANES), f32)
    loglik = jnp.zeros((1, LANES), f32)
    seen = jnp.zeros((1, LANES), f32)
    for half in range(halves):
        a = shifted[half * classes : (half + 1) * classes]
        top = jnp.max(a, axis=0, keepdims=True)
        total = top + jnp.log(jnp.sum(jnp.exp(a - top), axis=0, keepdims=True))
        n = counts_ref[pl.ds(g * halves + half, 1), :].astype(f32)
        result[half : half + 1, :] = total / taxa
        mass = mass + n * jnp.exp(a - total)
        loglik = loglik + n * total
        seen = seen + n
    for c in range(classes):
        part[c, 0:1] = mass[c : c + 1]
        part[c, 1:2] = loglik
        part[c, 2:3] = seen
        part[c, 3:4] = jnp.zeros_like(seen)
    own = g * site_devices + me
    for a, b in reversed(others):
        target = lax.rem(g + a, groups)
        pltpu.make_async_remote_copy(
            src_ref=part.at[target],
            dst_ref=part_got.at[own],
            send_sem=part_send,
            recv_sem=part_recv,
            device_id={"cls": target, "site": lax.rem(me + b, site_devices)},
            device_id_type=MESH,
        ).start()
    part_got[own] = part[g]
    arrivals = part_got.at[pl.ds(0, len(others))]
    pltpu.make_async_copy(arrivals, arrivals, part_recv).wait()
    sums = part_got[0]
    for d in range(1, groups * site_devices):
        sums = sums + part_got[d]
    line = jnp.sum(sums, axis=1, keepdims=True)
    all_count = line[2:3]
    mean = line[1:2] / (all_count * taxa)
    share = line[0:1] / all_count
    pltpu.make_async_copy(arrivals, arrivals, part_send).wait()
    result[halves : halves + 1, :] = jnp.broadcast_to(share, (1, LANES))
    result[halves + 1 : halves + 2, :] = jnp.broadcast_to(mean, (1, LANES))


def finish(result, site_out, weight_out, mean_out):
    halves = result.shape[0] - 2
    for half in range(halves):
        site_out[0:1, half * LANES : (half + 1) * LANES] = result[half : half + 1, :]
    weight_out[...] = result[halves : halves + 1, 0:1]
    mean_out[...] = result[halves + 1 : halves + 2, 0:1]


def solution(mesh):
    groups = mesh.shape["cls"]
    site_devices = mesh.shape["site"]

    def per_device(tip_codes, counts, children, lengths, frequencies, weights):
        local, sites = tip_codes.shape
        taxa = local * groups
        classes, branches = lengths.shape
        quarter = sites // groups
        halves = quarter // LANES
        rows = halves * classes
        low = LEVELS - TOP
        clades = local >> low
        low_rows = sum(local >> h for h in range(low))
        table_width = -(-(branches + 1) // LANES) * LANES
        up_count = branches - level_base(taxa, low)
        kids = children.T
        vmem = pl.BlockSpec(memory_space=pltpu.VMEM)
        smem = pl.BlockSpec(memory_space=pltpu.SMEM)
        f32 = jnp.float32
        result = pl.pallas_call(
            functools.partial(kernel, groups, site_devices),
            out_shape=jax.ShapeDtypeStruct((halves + 2, LANES), f32),
            in_specs=[pl.BlockSpec(memory_space=pl.ANY), vmem, vmem, smem, vmem, vmem, vmem],
            out_specs=vmem,
            scratch_shapes=[
                pltpu.VMEM((local, sites), jnp.int32),
                pltpu.VMEM((halves, local, LANES), f32),
                pltpu.VMEM((16, table_width), f32),
                pltpu.VMEM((classes, low_rows, LANES), f32),
                pltpu.VMEM((up_count, rows, LANES), f32),
                pltpu.VMEM((classes, 4, 8, LANES), f32),
                pltpu.VMEM((groups, clades * 3 + 1, rows, LANES), f32),
                pltpu.VMEM((groups, clades * 3 + 1, rows, LANES), f32),
                pltpu.VMEM((2 ** TOP, 4, rows, LANES), f32),
                pltpu.VMEM((classes, 4, LANES), f32),
                pltpu.VMEM((groups * site_devices, 4, LANES), f32),
                pltpu.SemaphoreType.DMA,
                pltpu.SemaphoreType.DMA((groups,)),
                pltpu.SemaphoreType.DMA((groups,)),
                pltpu.SemaphoreType.DMA,
                pltpu.SemaphoreType.DMA,
            ],
            compiler_params=pltpu.CompilerParams(collective_id=0, has_side_effects=True),
        )(
            tip_codes,
            counts.reshape(sites // LANES, LANES),
            kids,
            kids,
            lengths,
            frequencies,
            weights.reshape(1, classes),
        )
        site_loglik, new_weights, mean_loglik = pl.pallas_call(
            finish,
            out_shape=(
                jax.ShapeDtypeStruct((1, quarter), f32),
                jax.ShapeDtypeStruct((1, 1), f32),
                jax.ShapeDtypeStruct((1, 1), f32),
            ),
            in_specs=[vmem],
            out_specs=(vmem, vmem, vmem),
        )(result)
        return site_loglik, new_weights.reshape(1), mean_loglik.reshape(())

    return jax.shard_map(
        per_device,
        mesh=mesh,
        in_specs=(P("cls", "site"), P("site"), P(), P(), P(), P()),
        out_specs=(P("cls", "site"), P("cls"), P()),
        check_vma=False,
    )
```

```python
import functools

import jax
import jax.numpy as jnp
from jax import lax
from jax.experimental import pallas as pl
from jax.experimental.pallas import tpu as pltpu
from jax.sharding import PartitionSpec as P

LEVELS = 10
TOP = 4
LANES = 128
PIECES = 1
MESH = pl.DeviceIdType.MESH


def level_base(taxa, h):
    return 0 if h == 0 else 2 * taxa - (taxa >> (h - 1))


def look_up(table, index):
    numbers = lax.GatherDimensionNumbers(
        offset_dims=(),
        collapsed_slice_dims=(0,),
        start_index_map=(0,),
        operand_batching_dims=(1,),
        start_indices_batching_dims=(1,),
    )
    return lax.gather(
        table,
        index[..., None],
        numbers,
        (1, 1),
        mode=lax.GatherScatterMode.PROMISE_IN_BOUNDS,
    )


def kernel(
    groups,
    site_devices,
    codes_hbm,
    counts_hbm,
    kids_hbm,
    lengths_hbm,
    freq_hbm,
    weights_hbm,
    result,
    codes,
    counts,
    kids,
    lengths_ref,
    freq_ref,
    weights_ref,
    table,
    tail,
    grow,
    grow_up,
    stat,
    pick,
    pairs,
    mids,
    scale_sum,
    sent,
    got,
    sent_scale,
    got_scale,
    upper,
    part,
    part_got,
    in_sem,
    code_sem,
    send_sem,
    recv_sem,
    scale_send,
    scale_recv,
    part_send,
    part_recv,
):
    g = lax.axis_index("cls")
    me = lax.axis_index("site")
    tiles, folds, _, _ = codes.shape
    local = tiles * 8
    taxa = local * groups
    classes, branches = lengths_ref.shape
    halves = folds // groups
    low = LEVELS - TOP
    clades = local >> low
    rows = halves * classes
    f32 = jnp.float32

    copies = []
    small = [
        (freq_hbm, freq_ref),
        (lengths_hbm, lengths_ref),
        (kids_hbm, kids),
        (weights_hbm, weights_ref),
        (counts_hbm, counts),
    ]
    for n, (source, target) in enumerate(small):
        copies.append(pltpu.make_async_copy(source, target, in_sem.at[n]))
        copies[-1].start()
    fetches = []
    for fold in range(folds):
        lanes = pl.ds(fold * LANES, LANES)
        fetches.append(
            pltpu.make_async_copy(codes_hbm.at[:, :, lanes], codes.at[:, fold], code_sem.at[fold])
        )
        fetches[-1].start()

    barrier = pltpu.get_barrier_semaphore()
    others = [(a, b) for a in range(groups) for b in range(site_devices) if a or b]
    for a, b in others:
        pl.semaphore_signal(
            barrier,
            inc=1,
            device_id={"cls": lax.rem(g + a, groups), "site": lax.rem(me + b, site_devices)},
            device_id_type=MESH,
        )

    copies[0].wait()
    freq = freq_ref[...]
    pi = freq / jnp.sum(freq, axis=1, keepdims=True)
    beta = 1.0 / (1.0 - jnp.sum(pi * pi, axis=1, keepdims=True))
    for i in range(4):
        wide = jnp.broadcast_to(pi[:, i : i + 1], (classes, LANES))
        for c in range(classes):
            stat[c, i] = jnp.broadcast_to(wide[c : c + 1], (8, LANES))
    copies[1].wait()
    lengths = lengths_ref[...]
    r = jnp.exp(beta * lengths) - 1.0
    width = table.shape[1]
    wide_levels = [h for h in range(low) if (local >> h) % LANES == 0]
    tail_start = level_base(taxa, len(wide_levels)) // LANES * LANES
    table[0:classes, 0:branches] = r
    table[0:classes, branches:width] = jnp.zeros((classes, width - branches), f32)
    table[classes : 2 * classes, :] = jnp.zeros((classes, width), f32)
    table[classes : 2 * classes, tail_start : tail_start + 4] = pi
    table[classes : 2 * classes, tail_start + 4 : tail_start + 8] = pi
    tail[...] = table[:, tail_start:width].T
    for c in range(classes):
        pick[c] = jnp.broadcast_to(tail[0:8, classes + c : classes + c + 1], (8, LANES))
    offset = {}
    total_rows = 0
    for h in range(low):
        count = local >> h
        base = level_base(taxa, h)
        offset[h] = total_rows
        if h in wide_levels:
            span = pl.ds(pl.multiple_of(base + g * count, LANES), count)
            columns = table[:, span].T
        else:
            columns = tail[pl.ds(pl.multiple_of(base - tail_start + g * count, 8), count), :]
        for c in range(classes):
            grow[c, total_rows : total_rows + count, :] = jnp.broadcast_to(
                columns[:, c : c + 1], (count, LANES)
            )
        total_rows += count
    copies[2].wait()
    for fetch in fetches:
        fetch.wait()
    flat = codes.reshape(local * folds, LANES)

    def child_row(side, level, node):
        return kids[side, taxa - (taxa >> (level - 1)) + node]

    def factor(c, h, node):
        return grow[c, pl.ds(offset[h] + node, 1), :]

    def tip_codes(tip):
        return flat[pl.ds((tip >> 3) * (8 * folds) + (tip & 7), folds, stride=8), :]

    def spread(c, values, scale):
        mean = (values[0] * stat[c, 0] + values[1] * stat[c, 1]) + (
            values[2] * stat[c, 2] + values[3] * stat[c, 3]
        )
        move = scale * mean
        return [value + move for value in values], mean

    per = [(local >> h) // clades for h in range(low + 1)]
    span = classes // PIECES

    def step(index, carry):
        p = index // clades
        j = lax.rem(index, clades)
        mine = [span * p + n for n in range(span)]
        for n in range(per[1]):
            node = j * per[1] + n
            left = child_row(0, 1, g * (local >> 1) + node) & (local - 1)
            right = child_row(1, 1, g * (local >> 1) + node) & (local - 1)
            a = tip_codes(left)
            b = tip_codes(right)
            same = jnp.where(a == b, 1.0, 0.0)
            in_a = [a == i for i in range(4)]
            in_b = [b == i for i in range(4)]
            for q, c in enumerate(mine):
                pi_a = look_up(pick[c], a)
                pi_b = look_up(pick[c], b)
                off_a = factor(c, 0, left) * pi_a
                off_b = factor(c, 0, right) * pi_b
                on_b = off_b + same
                mean = off_a * (pi_b + off_b) + pi_a * on_b
                move = factor(c, 1, node) * mean
                at_a = (off_a + 1.0) * on_b + move
                at_b = (off_b + 1.0) * (off_a + same) + move
                rest = off_a * off_b + move
                for i in range(4):
                    pairs[n, 4 * q + i] = jnp.where(
                        in_a[i], at_a, jnp.where(in_b[i], at_b, rest)
                    )
        logs = [None] * span
        for n in range(per[3]):
            node = j * per[3] + n
            seconds = [
                child_row(side, 3, g * (local >> 3) + node) & (per[2] - 1) for side in (0, 1)
            ]
            firsts = [
                [
                    child_row(side, 2, g * (local >> 2) + j * per[2] + second) & (per[1] - 1)
                    for side in (0, 1)
                ]
                for second in seconds
            ]
            for q, c in enumerate(mine):
                both = []
                for second, first in zip(seconds, firsts):
                    values = [
                        pairs[first[0], 4 * q + i] * pairs[first[1], 4 * q + i] for i in range(4)
                    ]
                    both.append(spread(c, values, factor(c, 2, j * per[2] + second))[0])
                values = [x * y for x, y in zip(*both)]
                values, mean = spread(c, values, factor(c, 3, node))
                scale = pl.reciprocal(mean, approx=True)
                logs[q] = jnp.log(scale) if n == 0 else logs[q] + jnp.log(scale)
                for i in range(4):
                    mids[n, 4 * q + i] = values[i] * scale
        fourths = [
            [child_row(side, 5, g * (local >> 5) + j * per[5] + n) & (per[4] - 1) for side in (0, 1)]
            for n in range(per[5])
        ]
        thirds = [
            [
                [
                    child_row(side, 4, g * (local >> 4) + j * per[4] + fourth) & (per[3] - 1)
                    for side in (0, 1)
                ]
                for fourth in pair
            ]
            for pair in fourths
        ]
        for q, c in enumerate(mine):
            top = []
            for n in range(per[5]):
                both = []
                for fourth, third in zip(fourths[n], thirds[n]):
                    values = [
                        mids[third[0], 4 * q + i] * mids[third[1], 4 * q + i] for i in range(4)
                    ]
                    both.append(spread(c, values, factor(c, 4, j * per[4] + fourth))[0])
                values = [x * y for x, y in zip(*both)]
                top.append(spread(c, values, factor(c, 5, j * per[5] + n))[0])
            values = [x * y for x, y in zip(*top)]
            inverse = 1.0 / values[3]
            for i in range(3):
                ratio = values[i] * inverse
                for block in range(groups):
                    sent[block, p, j, i, halves * q : halves * (q + 1), :] = ratio[
                        halves * block : halves * (block + 1)
                    ]
            before = jnp.where(j == 0, 0.0, scale_sum[q])
            total = before + (jnp.log(values[3]) - logs[q])
            scale_sum[q] = total
            for block in range(groups):
                sent_scale[block, p, halves * q : halves * (q + 1), :] = total[
                    halves * block : halves * (block + 1)
                ]

        @pl.when(index == 0)
        def _():
            pl.semaphore_wait(barrier, len(others))

        for slot in order:
            target = partner(slot)
            pltpu.make_async_remote_copy(
                src_ref=sent.at[target, p, j],
                dst_ref=got.at[slot, p, j],
                send_sem=send_sem,
                recv_sem=recv_sem,
                device_id={"cls": target},
                device_id_type=MESH,
            ).start()

        @pl.when(j == clades - 1)
        def _():
            for slot in order:
                target = partner(slot)
                pltpu.make_async_remote_copy(
                    src_ref=sent_scale.at[target, p],
                    dst_ref=got_scale.at[slot, p],
                    send_sem=scale_send,
                    recv_sem=scale_recv,
                    device_id={"cls": target},
                    device_id_type=MESH,
                ).start()

        return carry

    xor = groups & (groups - 1) == 0
    order = [2, 3, 1] if groups == 4 else list(range(1, groups))

    def partner(slot):
        return g ^ slot if xor else lax.rem(g + slot, groups)

    def slot_of(source):
        return g ^ source if xor else lax.rem(source + groups - g, groups)

    lax.fori_loop(0, PIECES * clades, step, 0)
    got[0] = sent[g]
    got_scale[0] = sent_scale[g]
    first_up = level_base(taxa, low)
    window = first_up // LANES * LANES
    r8 = jnp.concatenate([r[n // halves : n // halves + 1, window:] for n in range(rows)], axis=0)
    for j in range(branches - first_up):
        at = first_up - window + j
        grow_up[j] = jnp.broadcast_to(r8[:, at : at + 1], (rows, LANES))
    drift = beta * jnp.sum(lengths, axis=1, keepdims=True)
    for copy in copies[3:]:
        copy.wait()
    arrived = got.at[pl.ds(1, groups - 1)]
    pltpu.make_async_copy(arrived, arrived, recv_sem).wait()
    scales_arrived = got_scale.at[pl.ds(1, groups - 1)]
    pltpu.make_async_copy(scales_arrived, scales_arrived, scale_recv).wait()

    def whole(*parts):
        return parts[0] if len(parts) == 1 else jnp.concatenate(parts, axis=0)

    pis8 = [
        jnp.concatenate([stat[n // halves, i, 0:1] for n in range(rows)], axis=0) for i in range(4)
    ]
    scales = functools.reduce(jnp.add, [whole(*[got_scale[k, p] for p in range(PIECES)]) for k in range(groups)])

    def child(tree_level, ident):
        if tree_level == low:
            place = (ident - first_up) & (2**TOP - 1)
            k = slot_of(place // clades)
            j = lax.rem(place, clades)
            values = [whole(*[got[k, p, j, i] for p in range(PIECES)]) for i in range(3)]
            values.append(jnp.ones((rows, LANES), f32))
        else:
            at = jnp.clip(ident - level_base(taxa, low + 1), 0, 2**TOP - 1)
            values = [upper[at, i] for i in range(4)]
        mean = (values[0] * pis8[0] + values[1] * pis8[1]) + (
            values[2] * pis8[2] + values[3] * pis8[3]
        )
        move = grow_up[jnp.clip(ident - first_up, 0, branches - first_up - 1)] * mean
        return [value + move for value in values]

    place = 0
    for tree_level in range(low, LEVELS):
        count = taxa >> (tree_level + 1)
        first = taxa - (taxa >> tree_level)
        for n in range(count):
            left = child(tree_level, kids[0, first + n])
            right = child(tree_level, kids[1, first + n])
            values = [a * b for a, b in zip(left, right)]
            largest = jnp.maximum(
                jnp.maximum(values[0], values[1]), jnp.maximum(values[2], values[3])
            )
            scale = pl.reciprocal(largest, approx=True)
            scales = scales - jnp.log(scale)
            values = [value * scale for value in values]
            if tree_level < LEVELS - 1:
                for i in range(4):
                    upper[place, i] = values[i]
                place += 1
    end = (values[0] * pis8[0] + values[1] * pis8[1]) + (
        values[2] * pis8[2] + values[3] * pis8[3]
    )
    spot = lax.broadcasted_iota(jnp.int32, (classes, classes), 0)
    spot = spot == lax.broadcasted_iota(jnp.int32, (classes, classes), 1)
    weights = jnp.sum(jnp.where(spot, weights_ref[...], 0.0), axis=1, keepdims=True)
    log_weight = jnp.log(weights / jnp.sum(weights, axis=0, keepdims=True))
    bias = log_weight - drift
    bias = jnp.concatenate([bias[n // halves : n // halves + 1] for n in range(rows)], axis=0)
    shifted = scales + jnp.log(end) + bias
    each = [shifted[halves * c : halves * (c + 1)] for c in range(classes)]
    top = functools.reduce(jnp.maximum, each)
    total = top + jnp.log(functools.reduce(jnp.add, [jnp.exp(a - top) for a in each]))
    result[0:halves, :] = total / taxa
    n = counts[pl.ds(g * halves, halves), :].astype(f32)

    def over_halves(x):
        return functools.reduce(jnp.add, [x[h : h + 1] for h in range(halves)])

    loglik = over_halves(n * total)
    seen = over_halves(n)
    sums = [over_halves(n * jnp.exp(a - total)) for a in each] + [loglik, seen]
    size = len(sums)
    sums = jnp.sum(jnp.concatenate(sums, axis=0), axis=1, keepdims=True)
    lane = lax.broadcasted_iota(jnp.int32, (size, LANES), 1)
    spot = lane == lax.broadcasted_iota(jnp.int32, (size, LANES), 0)
    part[...] = jnp.sum(jnp.where(spot, sums, 0.0), axis=0, keepdims=True)
    own = g * site_devices + me
    for a, b in reversed(others):
        pltpu.make_async_remote_copy(
            src_ref=part,
            dst_ref=part_got.at[own],
            send_sem=part_send,
            recv_sem=part_recv,
            device_id={"cls": lax.rem(g + a, groups), "site": lax.rem(me + b, site_devices)},
            device_id_type=MESH,
        ).start()
    part_got[own] = part[...]
    arrivals = part_got.at[pl.ds(0, len(others))]
    pltpu.make_async_copy(arrivals, arrivals, part_recv).wait()
    line = [part_got[d] for d in range(groups * site_devices)]
    while len(line) > 1:
        line = [jnp.add(*line[d : d + 2]) if d + 1 < len(line) else line[d] for d in range(0, len(line), 2)]
    lane = lax.broadcasted_iota(jnp.int32, (3, LANES), 1)
    row = lax.broadcasted_iota(jnp.int32, (3, LANES), 0)
    spot = lane == jnp.where(row == 0, g, classes - 1 + row)
    line = jnp.sum(jnp.where(spot, line[0], 0.0), axis=1, keepdims=True)
    all_count = line[2:3]
    mean = line[1:2] / (all_count * taxa)
    share = line[0:1] / all_count
    pltpu.make_async_copy(arrivals, arrivals, part_send).wait()
    pltpu.make_async_copy(arrived, arrived, send_sem).wait()
    pltpu.make_async_copy(scales_arrived, scales_arrived, scale_send).wait()
    result[halves : halves + 1, :] = jnp.broadcast_to(share, (1, LANES))
    result[halves + 1 : halves + 2, :] = jnp.broadcast_to(mean, (1, LANES))


def finish(result, site_out, weight_out, mean_out):
    halves = result.shape[0] - 2
    for half in range(halves):
        site_out[0:1, half * LANES : (half + 1) * LANES] = result[half : half + 1, :]
    weight_out[...] = result[halves : halves + 1, 0:1]
    mean_out[...] = result[halves + 1 : halves + 2, 0:1]


def solution(mesh):
    groups = mesh.shape["cls"]
    site_devices = mesh.shape["site"]

    def per_device(tip_codes, counts, children, lengths, frequencies, weights):
        local, sites = tip_codes.shape
        taxa = local * groups
        classes, branches = lengths.shape
        quarter = sites // groups
        halves = quarter // LANES
        rows = halves * classes
        low = LEVELS - TOP
        clades = local >> low
        low_rows = sum(local >> h for h in range(low))
        table_width = -(-branches // LANES) * LANES
        wide_levels = [h for h in range(low) if (local >> h) % LANES == 0]
        tail_start = level_base(taxa, len(wide_levels)) // LANES * LANES
        folds = sites // LANES
        up_count = branches - level_base(taxa, low)
        kids = children.T
        vmem = pl.BlockSpec(memory_space=pltpu.VMEM)
        hbm = pl.BlockSpec(memory_space=pltpu.HBM)
        f32 = jnp.float32
        result = pl.pallas_call(
            functools.partial(kernel, groups, site_devices),
            out_shape=jax.ShapeDtypeStruct((halves + 2, LANES), f32),
            in_specs=[hbm] * 6,
            out_specs=vmem,
            scratch_shapes=[
                pltpu.VMEM((local // 8, folds, 8, LANES), jnp.int32),
                pltpu.VMEM((folds, LANES), jnp.int32),
                pltpu.SMEM(kids.shape, jnp.int32),
                pltpu.VMEM(lengths.shape, f32),
                pltpu.VMEM(frequencies.shape, f32),
                pltpu.VMEM((1, classes), f32),
                pltpu.VMEM((8, table_width), f32),
                pltpu.VMEM((table_width - tail_start, 8), f32),
                pltpu.VMEM((classes, low_rows, LANES), f32),
                pltpu.VMEM((up_count, rows, LANES), f32),
                pltpu.VMEM((classes, 4, 8, LANES), f32),
                pltpu.VMEM((classes, 8, LANES), f32),
                pltpu.VMEM(((local >> 1) // clades, 4 * classes // PIECES, folds, LANES), f32),
                pltpu.VMEM(((local >> 3) // clades, 4 * classes // PIECES, folds, LANES), f32),
                pltpu.VMEM((classes // PIECES, folds, LANES), f32),
                pltpu.VMEM((groups, PIECES, clades, 3, rows // PIECES, LANES), f32),
                pltpu.VMEM((groups, PIECES, clades, 3, rows // PIECES, LANES), f32),
                pltpu.VMEM((groups, PIECES, rows // PIECES, LANES), f32),
                pltpu.VMEM((groups, PIECES, rows // PIECES, LANES), f32),
                pltpu.VMEM((2 ** TOP, 4, rows, LANES), f32),
                pltpu.VMEM((1, LANES), f32),
                pltpu.VMEM((groups * site_devices, 1, LANES), f32),
                pltpu.SemaphoreType.DMA((5,)),
                pltpu.SemaphoreType.DMA((folds,)),
                pltpu.SemaphoreType.DMA,
                pltpu.SemaphoreType.DMA,
                pltpu.SemaphoreType.DMA,
                pltpu.SemaphoreType.DMA,
                pltpu.SemaphoreType.DMA,
                pltpu.SemaphoreType.DMA,
            ],
            compiler_params=pltpu.CompilerParams(collective_id=0, has_side_effects=True, vmem_limit_bytes=56549376),
        )(
            tip_codes.reshape(local // 8, 8, sites),
            counts.reshape(folds, LANES),
            kids,
            lengths,
            frequencies,
            weights.reshape(1, classes),
        )
        site_loglik, new_weights, mean_loglik = pl.pallas_call(
            finish,
            out_shape=(
                jax.ShapeDtypeStruct((1, quarter), f32),
                jax.ShapeDtypeStruct((1, 1), f32),
                jax.ShapeDtypeStruct((1, 1), f32),
            ),
            in_specs=[vmem],
            out_specs=(vmem, vmem, vmem),
            compiler_params=pltpu.CompilerParams(vmem_limit_bytes=1 << 20),
        )(result)
        return site_loglik, new_weights.reshape(1), mean_loglik.reshape(())

    return jax.shard_map(
        per_device,
        mesh=mesh,
        in_specs=(P("cls", "site"), P("site"), P(), P(), P(), P()),
        out_specs=(P("cls", "site"), P("cls"), P()),
        check_vma=False,
    )
```

```python
import functools

import jax
import jax.numpy as jnp
from jax import lax
from jax.experimental import pallas as pl
from jax.experimental.pallas import tpu as pltpu
from jax.sharding import PartitionSpec as P

LEVELS = 10
TOP = 4
LANES = 128
PIECES = 1
MESH = pl.DeviceIdType.MESH


def level_base(taxa, h):
    return 0 if h == 0 else 2 * taxa - (taxa >> (h - 1))


def look_up(table, index):
    numbers = lax.GatherDimensionNumbers(
        offset_dims=(),
        collapsed_slice_dims=(0,),
        start_index_map=(0,),
        operand_batching_dims=(1,),
        start_indices_batching_dims=(1,),
    )
    return lax.gather(
        table,
        index[..., None],
        numbers,
        (1, 1),
        mode=lax.GatherScatterMode.PROMISE_IN_BOUNDS,
    )


def kernel(
    groups,
    site_devices,
    codes_hbm,
    counts_hbm,
    kids_hbm,
    lengths_hbm,
    freq_hbm,
    weights_hbm,
    result,
    codes,
    counts,
    kids,
    lengths_ref,
    freq_ref,
    weights_ref,
    table,
    columns,
    tail,
    grow,
    grow_up,
    stat,
    pick,
    pairs,
    mids,
    scale_sum,
    sent,
    got,
    sent_scale,
    got_scale,
    upper,
    part,
    part_got,
    in_sem,
    code_sem,
    send_sem,
    recv_sem,
    scale_send,
    scale_recv,
    part_send,
    part_recv,
):
    g = lax.axis_index("cls")
    me = lax.axis_index("site")
    tiles, folds, _, _ = codes.shape
    local = tiles * 8
    taxa = local * groups
    classes, branches = lengths_ref.shape
    halves = folds // groups
    low = LEVELS - TOP
    clades = local >> low
    rows = halves * classes
    f32 = jnp.float32

    copies = []
    small = [
        (freq_hbm, freq_ref),
        (lengths_hbm, lengths_ref),
        (kids_hbm, kids),
        (weights_hbm, weights_ref),
        (counts_hbm, counts),
    ]
    for n, (source, target) in enumerate(small):
        copies.append(pltpu.make_async_copy(source, target, in_sem.at[n]))
        copies[-1].start()
    fetches = []
    for fold in range(folds):
        lanes = pl.ds(fold * LANES, LANES)
        fetches.append(
            pltpu.make_async_copy(codes_hbm.at[:, :, lanes], codes.at[:, fold], code_sem.at[fold])
        )
        fetches[-1].start()

    barrier = pltpu.get_barrier_semaphore()
    others = [(a, b) for a in range(groups) for b in range(site_devices) if a or b]
    for a, b in others:
        pl.semaphore_signal(
            barrier,
            inc=1,
            device_id={"cls": lax.rem(g + a, groups), "site": lax.rem(me + b, site_devices)},
            device_id_type=MESH,
        )

    copies[0].wait()
    freq = [jnp.broadcast_to(freq_ref[:, i : i + 1], (classes, LANES)) for i in range(4)]
    whole_freq = (freq[0] + freq[1]) + (freq[2] + freq[3])
    pi = [own / whole_freq for own in freq]
    beta = 1.0 / (1.0 - ((pi[0] * pi[0] + pi[1] * pi[1]) + (pi[2] * pi[2] + pi[3] * pi[3])))
    width = table.shape[1]
    table[classes:8, :] = jnp.zeros((8 - classes, width), f32)
    for c in range(classes):
        for i in range(4):
            stat[c, i] = jnp.broadcast_to(pi[i][c : c + 1], (8, LANES))
            pick[c, i : i + 1] = pi[i][c : c + 1]
            pick[c, i + 4 : i + 5] = pi[i][c : c + 1]
    copies[1].wait()
    for at in range(0, width, LANES):
        end = min(at + LANES, branches)
        table[0:classes, at:end] = jnp.exp(beta[:, : end - at] * lengths_ref[:, at:end]) - 1.0
    wide_levels = [h for h in range(low) if (local >> h) % LANES == 0]
    tail_start = level_base(taxa, len(wide_levels)) // LANES * LANES
    offset = {}
    total_rows = 0
    for h in range(low):
        count = local >> h
        offset[h] = total_rows
        if h in wide_levels:
            here = pl.ds(pl.multiple_of(level_base(taxa, h) + g * count, LANES), count)
            columns[total_rows : total_rows + count, :] = table[:, here].T
        total_rows += count
    tail[...] = table[:, tail_start:width].T
    per = [(local >> h) // clades for h in range(low + 1)]

    def fill(h, start, count):
        if h in wide_levels:
            column = columns[pl.ds(pl.multiple_of(offset[h] + start, 8), count), :]
        else:
            base = level_base(taxa, h) - tail_start + g * (local >> h)
            column = tail[pl.ds(pl.multiple_of(base + start, 8), count), :]
        target = pl.ds(pl.multiple_of(offset[h] + start, 8), count)
        for c in range(classes):
            grow[c, target, :] = jnp.broadcast_to(column[:, c : c + 1], (count, LANES))

    for h in range(low):
        fill(h, 0, local >> h)
    copies[2].wait()
    for fetch in fetches:
        fetch.wait()
    flat = codes.reshape(local * folds, LANES)

    def child_row(side, level, node):
        return kids[side, taxa - (taxa >> (level - 1)) + node]

    def factor(c, h, node):
        return grow[c, pl.ds(offset[h] + node, 1), :]

    def tip_codes(tip):
        return flat[pl.ds((tip >> 3) * (8 * folds) + (tip & 7), folds, stride=8), :]

    def spread(c, values, scale):
        mean = (values[0] * stat[c, 0] + values[1] * stat[c, 1]) + (
            values[2] * stat[c, 2] + values[3] * stat[c, 3]
        )
        move = scale * mean
        return [value + move for value in values], mean

    span = classes // PIECES

    def step(index, carry):
        p = index // clades
        j = lax.rem(index, clades)
        mine = [span * p + n for n in range(span)]
        for n in range(per[1]):
            node = j * per[1] + n
            left = child_row(0, 1, g * (local >> 1) + node) & (local - 1)
            right = child_row(1, 1, g * (local >> 1) + node) & (local - 1)
            a = tip_codes(left)
            b = tip_codes(right)
            same = jnp.where(a == b, 1.0, 0.0)
            in_a = [a == i for i in range(4)]
            in_b = [b == i for i in range(4)]
            for q, c in enumerate(mine):
                pi_a = look_up(pick[c], a)
                pi_b = look_up(pick[c], b)
                off_a = factor(c, 0, left) * pi_a
                off_b = factor(c, 0, right) * pi_b
                on_b = off_b + same
                mean = off_a * (pi_b + off_b) + pi_a * on_b
                move = factor(c, 1, node) * mean
                at_a = (off_a + 1.0) * on_b + move
                at_b = (off_b + 1.0) * (off_a + same) + move
                rest = off_a * off_b + move
                for i in range(4):
                    pairs[n, 4 * q + i] = jnp.where(
                        in_a[i], at_a, jnp.where(in_b[i], at_b, rest)
                    )
        logs = [None] * span
        for n in range(per[3]):
            node = j * per[3] + n
            seconds = [
                child_row(side, 3, g * (local >> 3) + node) & (per[2] - 1) for side in (0, 1)
            ]
            firsts = [
                [
                    child_row(side, 2, g * (local >> 2) + j * per[2] + second) & (per[1] - 1)
                    for side in (0, 1)
                ]
                for second in seconds
            ]
            for q, c in enumerate(mine):
                both = []
                for second, first in zip(seconds, firsts):
                    values = [
                        pairs[first[0], 4 * q + i] * pairs[first[1], 4 * q + i] for i in range(4)
                    ]
                    both.append(spread(c, values, factor(c, 2, j * per[2] + second))[0])
                values = [x * y for x, y in zip(*both)]
                values, mean = spread(c, values, factor(c, 3, node))
                scale = pl.reciprocal(mean, approx=True)
                logs[q] = jnp.log(scale) if n == 0 else logs[q] + jnp.log(scale)
                for i in range(4):
                    mids[n, 4 * q + i] = values[i] * scale
        fourths = [
            [child_row(side, 5, g * (local >> 5) + j * per[5] + n) & (per[4] - 1) for side in (0, 1)]
            for n in range(per[5])
        ]
        thirds = [
            [
                [
                    child_row(side, 4, g * (local >> 4) + j * per[4] + fourth) & (per[3] - 1)
                    for side in (0, 1)
                ]
                for fourth in pair
            ]
            for pair in fourths
        ]
        for q, c in enumerate(mine):
            top = []
            for n in range(per[5]):
                both = []
                for fourth, third in zip(fourths[n], thirds[n]):
                    values = [
                        mids[third[0], 4 * q + i] * mids[third[1], 4 * q + i] for i in range(4)
                    ]
                    both.append(spread(c, values, factor(c, 4, j * per[4] + fourth))[0])
                values = [x * y for x, y in zip(*both)]
                top.append(spread(c, values, factor(c, 5, j * per[5] + n))[0])
            values = [x * y for x, y in zip(*top)]
            inverse = 1.0 / values[3]
            for i in range(3):
                ratio = values[i] * inverse
                for block in range(groups):
                    sent[block, p, j, i, halves * q : halves * (q + 1), :] = ratio[
                        halves * block : halves * (block + 1)
                    ]
            before = jnp.where(j == 0, 0.0, scale_sum[q])
            total = before + (jnp.log(values[3]) - logs[q])
            scale_sum[q] = total
            for block in range(groups):
                sent_scale[block, p, halves * q : halves * (q + 1), :] = total[
                    halves * block : halves * (block + 1)
                ]

        @pl.when(index == 0)
        def _():
            pl.semaphore_wait(barrier, len(others))

        for slot in order:
            target = partner(slot)
            pltpu.make_async_remote_copy(
                src_ref=sent.at[target, p, j],
                dst_ref=got.at[slot, p, j],
                send_sem=send_sem,
                recv_sem=recv_sem,
                device_id={"cls": target},
                device_id_type=MESH,
            ).start()

        @pl.when(j == clades - 1)
        def _():
            for slot in order:
                target = partner(slot)
                pltpu.make_async_remote_copy(
                    src_ref=sent_scale.at[target, p],
                    dst_ref=got_scale.at[slot, p],
                    send_sem=scale_send,
                    recv_sem=scale_recv,
                    device_id={"cls": target},
                    device_id_type=MESH,
                ).start()

        return carry

    xor = groups & (groups - 1) == 0
    order = [2, 3, 1] if groups == 4 else list(range(1, groups))

    def partner(slot):
        return g ^ slot if xor else lax.rem(g + slot, groups)

    def slot_of(source):
        return g ^ source if xor else lax.rem(source + groups - g, groups)

    lax.fori_loop(0, PIECES * clades, step, 0)
    got[0] = sent[g]
    got_scale[0] = sent_scale[g]
    first_up = level_base(taxa, low)
    window = first_up // LANES * LANES
    r8 = jnp.concatenate([table[n // halves : n // halves + 1, window:branches] for n in range(rows)], axis=0)
    for j in range(branches - first_up):
        at = first_up - window + j
        grow_up[j] = jnp.broadcast_to(r8[:, at : at + 1], (rows, LANES))
    drift = beta[:, 0:1] * jnp.sum(lengths_ref[...], axis=1, keepdims=True)
    for copy in copies[3:]:
        copy.wait()
    pis8 = [
        jnp.concatenate([stat[n // halves, i, 0:1] for n in range(rows)], axis=0) for i in range(4)
    ]
    spot = lax.broadcasted_iota(jnp.int32, (classes, classes), 0)
    spot = spot == lax.broadcasted_iota(jnp.int32, (classes, classes), 1)
    weights = jnp.sum(jnp.where(spot, weights_ref[...], 0.0), axis=1, keepdims=True)
    log_weight = jnp.log(weights / jnp.sum(weights, axis=0, keepdims=True))
    bias = log_weight - drift
    bias = jnp.concatenate([bias[n // halves : n // halves + 1] for n in range(rows)], axis=0)
    seen_at = counts[pl.ds(g * halves, halves), :].astype(f32)
    def over_halves(x):
        return functools.reduce(jnp.add, [x[h : h + 1] for h in range(halves)])

    seen = over_halves(seen_at)
    arrived = got.at[pl.ds(1, groups - 1)]
    pltpu.make_async_copy(arrived, arrived, recv_sem).wait()
    scales_arrived = got_scale.at[pl.ds(1, groups - 1)]
    pltpu.make_async_copy(scales_arrived, scales_arrived, scale_recv).wait()

    def whole(*parts):
        return parts[0] if len(parts) == 1 else jnp.concatenate(parts, axis=0)

    scales = functools.reduce(jnp.add, [whole(*[got_scale[k, p] for p in range(PIECES)]) for k in range(groups)])

    def child(tree_level, ident):
        if tree_level == low:
            place = (ident - first_up) & (2**TOP - 1)
            k = slot_of(place // clades)
            j = lax.rem(place, clades)
            values = [whole(*[got[k, p, j, i] for p in range(PIECES)]) for i in range(3)]
            values.append(jnp.ones((rows, LANES), f32))
        else:
            at = jnp.clip(ident - level_base(taxa, low + 1), 0, 2**TOP - 1)
            values = [upper[at, i] for i in range(4)]
        mean = (values[0] * pis8[0] + values[1] * pis8[1]) + (
            values[2] * pis8[2] + values[3] * pis8[3]
        )
        move = grow_up[jnp.clip(ident - first_up, 0, branches - first_up - 1)] * mean
        return [value + move for value in values]

    place = 0
    for tree_level in range(low, LEVELS):
        count = taxa >> (tree_level + 1)
        first = taxa - (taxa >> tree_level)
        for n in range(count):
            left = child(tree_level, kids[0, first + n])
            right = child(tree_level, kids[1, first + n])
            values = [a * b for a, b in zip(left, right)]
            largest = jnp.maximum(
                jnp.maximum(values[0], values[1]), jnp.maximum(values[2], values[3])
            )
            scale = pl.reciprocal(largest, approx=True)
            scales = scales - jnp.log(scale)
            values = [value * scale for value in values]
            if tree_level < LEVELS - 1:
                for i in range(4):
                    upper[place, i] = values[i]
                place += 1
    end = (values[0] * pis8[0] + values[1] * pis8[1]) + (
        values[2] * pis8[2] + values[3] * pis8[3]
    )
    shifted = scales + jnp.log(end) + bias
    each = [shifted[halves * c : halves * (c + 1)] for c in range(classes)]
    top = functools.reduce(jnp.maximum, each)
    total = top + jnp.log(functools.reduce(jnp.add, [jnp.exp(a - top) for a in each]))
    result[0:halves, :] = total / taxa

    loglik = over_halves(seen_at * total)
    sums = [over_halves(seen_at * jnp.exp(a - total)) for a in each] + [loglik, seen]
    size = len(sums)
    sums = jnp.sum(jnp.concatenate(sums, axis=0), axis=1, keepdims=True)
    lane = lax.broadcasted_iota(jnp.int32, (size, LANES), 1)
    spot = lane == lax.broadcasted_iota(jnp.int32, (size, LANES), 0)
    part[...] = jnp.sum(jnp.where(spot, sums, 0.0), axis=0, keepdims=True)
    own = g * site_devices + me
    for a, b in reversed(others):
        pltpu.make_async_remote_copy(
            src_ref=part,
            dst_ref=part_got.at[own],
            send_sem=part_send,
            recv_sem=part_recv,
            device_id={"cls": lax.rem(g + a, groups), "site": lax.rem(me + b, site_devices)},
            device_id_type=MESH,
        ).start()
    part_got[own] = part[...]
    arrivals = part_got.at[pl.ds(0, len(others))]
    pltpu.make_async_copy(arrivals, arrivals, part_recv).wait()
    line = [part_got[d] for d in range(groups * site_devices)]
    while len(line) > 1:
        line = [jnp.add(*line[d : d + 2]) if d + 1 < len(line) else line[d] for d in range(0, len(line), 2)]
    lane = lax.broadcasted_iota(jnp.int32, (3, LANES), 1)
    row = lax.broadcasted_iota(jnp.int32, (3, LANES), 0)
    spot = lane == jnp.where(row == 0, g, classes - 1 + row)
    line = jnp.sum(jnp.where(spot, line[0], 0.0), axis=1, keepdims=True)
    all_count = line[2:3]
    mean = line[1:2] / (all_count * taxa)
    share = line[0:1] / all_count
    pltpu.make_async_copy(arrivals, arrivals, part_send).wait()
    pltpu.make_async_copy(arrived, arrived, send_sem).wait()
    pltpu.make_async_copy(scales_arrived, scales_arrived, scale_send).wait()
    result[halves : halves + 1, :] = jnp.broadcast_to(share, (1, LANES))
    result[halves + 1 : halves + 2, :] = jnp.broadcast_to(mean, (1, LANES))


def finish(result, site_out, weight_out, mean_out):
    halves = result.shape[0] - 2
    for half in range(halves):
        site_out[0:1, half * LANES : (half + 1) * LANES] = result[half : half + 1, :]
    weight_out[...] = result[halves : halves + 1, 0:1]
    mean_out[...] = result[halves + 1 : halves + 2, 0:1]


def solution(mesh):
    groups = mesh.shape["cls"]
    site_devices = mesh.shape["site"]

    def per_device(tip_codes, counts, children, lengths, frequencies, weights):
        local, sites = tip_codes.shape
        taxa = local * groups
        classes, branches = lengths.shape
        quarter = sites // groups
        halves = quarter // LANES
        rows = halves * classes
        low = LEVELS - TOP
        clades = local >> low
        low_rows = sum(local >> h for h in range(low))
        table_width = -(-branches // LANES) * LANES
        wide_levels = [h for h in range(low) if (local >> h) % LANES == 0]
        tail_start = level_base(taxa, len(wide_levels)) // LANES * LANES
        folds = sites // LANES
        up_count = branches - level_base(taxa, low)
        kids = children.T
        vmem = pl.BlockSpec(memory_space=pltpu.VMEM)
        hbm = pl.BlockSpec(memory_space=pltpu.HBM)
        f32 = jnp.float32
        result = pl.pallas_call(
            functools.partial(kernel, groups, site_devices),
            out_shape=jax.ShapeDtypeStruct((halves + 2, LANES), f32),
            in_specs=[hbm] * 6,
            out_specs=vmem,
            scratch_shapes=[
                pltpu.VMEM((local // 8, folds, 8, LANES), jnp.int32),
                pltpu.VMEM((folds, LANES), jnp.int32),
                pltpu.SMEM(kids.shape, jnp.int32),
                pltpu.VMEM(lengths.shape, f32),
                pltpu.VMEM(frequencies.shape, f32),
                pltpu.VMEM((1, classes), f32),
                pltpu.VMEM((8, table_width), f32),
                pltpu.VMEM((sum(local >> h for h in wide_levels), 8), f32),
                pltpu.VMEM((table_width - tail_start, 8), f32),
                pltpu.VMEM((classes, low_rows, LANES), f32),
                pltpu.VMEM((up_count, rows, LANES), f32),
                pltpu.VMEM((classes, 4, 8, LANES), f32),
                pltpu.VMEM((classes, 8, LANES), f32),
                pltpu.VMEM(((local >> 1) // clades, 4 * classes // PIECES, folds, LANES), f32),
                pltpu.VMEM(((local >> 3) // clades, 4 * classes // PIECES, folds, LANES), f32),
                pltpu.VMEM((classes // PIECES, folds, LANES), f32),
                pltpu.VMEM((groups, PIECES, clades, 3, rows // PIECES, LANES), f32),
                pltpu.VMEM((groups, PIECES, clades, 3, rows // PIECES, LANES), f32),
                pltpu.VMEM((groups, PIECES, rows // PIECES, LANES), f32),
                pltpu.VMEM((groups, PIECES, rows // PIECES, LANES), f32),
                pltpu.VMEM((2 ** TOP, 4, rows, LANES), f32),
                pltpu.VMEM((1, LANES), f32),
                pltpu.VMEM((groups * site_devices, 1, LANES), f32),
                pltpu.SemaphoreType.DMA((5,)),
                pltpu.SemaphoreType.DMA((folds,)),
                pltpu.SemaphoreType.DMA,
                pltpu.SemaphoreType.DMA,
                pltpu.SemaphoreType.DMA,
                pltpu.SemaphoreType.DMA,
                pltpu.SemaphoreType.DMA,
                pltpu.SemaphoreType.DMA,
            ],
            compiler_params=pltpu.CompilerParams(collective_id=0, has_side_effects=True, vmem_limit_bytes=32 << 20),
        )(
            *(
                pltpu.with_memory_space_constraint(operand, pltpu.HBM)
                for operand in (
                    tip_codes.reshape(local // 8, 8, sites),
                    counts.reshape(folds, LANES),
                    kids,
                    lengths,
                    frequencies,
                    weights.reshape(1, classes),
                )
            )
        )
        site_loglik, new_weights, mean_loglik = pl.pallas_call(
            finish,
            out_shape=(
                jax.ShapeDtypeStruct((1, quarter), f32),
                jax.ShapeDtypeStruct((1, 1), f32),
                jax.ShapeDtypeStruct((1, 1), f32),
            ),
            in_specs=[vmem],
            out_specs=(vmem, vmem, vmem),
            compiler_params=pltpu.CompilerParams(vmem_limit_bytes=1 << 20),
        )(result)
        return site_loglik, new_weights.reshape(1), mean_loglik.reshape(())

    return jax.shard_map(
        per_device,
        mesh=mesh,
        in_specs=(P("cls", "site"), P("site"), P(), P(), P(), P()),
        out_specs=(P("cls", "site"), P("cls"), P()),
        check_vma=False,
    )
```

```python
import functools

import jax
import jax.numpy as jnp
from jax import lax
from jax.experimental import pallas as pl
from jax.experimental.pallas import tpu as pltpu
from jax.sharding import PartitionSpec as P

LEVELS = 10
TOP = 4
LANES = 128
PIECES = 1
SIDES = 2
MESH = pl.DeviceIdType.MESH


def level_base(taxa, h):
    return 0 if h == 0 else 2 * taxa - (taxa >> (h - 1))


def look_up(table, index):
    numbers = lax.GatherDimensionNumbers(
        offset_dims=(),
        collapsed_slice_dims=(0,),
        start_index_map=(0,),
        operand_batching_dims=(1,),
        start_indices_batching_dims=(1,),
    )
    return lax.gather(
        table,
        index[..., None],
        numbers,
        (1, 1),
        mode=lax.GatherScatterMode.PROMISE_IN_BOUNDS,
    )


def kernel(
    groups,
    site_devices,
    codes_hbm,
    counts_hbm,
    kids_hbm,
    lengths_hbm,
    freq_hbm,
    weights_hbm,
    result,
    codes,
    counts,
    kids,
    lengths_ref,
    freq_ref,
    weights_ref,
    table,
    columns,
    tail,
    grow,
    grow_up,
    stat,
    pick,
    pairs,
    mids,
    scale_sum,
    sent,
    got,
    sent_scale,
    got_scale,
    upper,
    counts_got,
    site_sent,
    site_got,
    part,
    part_got,
    part_sink,
    in_sem,
    code_sem,
    send_sem,
    recv_sem,
    scale_send,
    scale_recv,
    part_send,
    part_recv,
    counts_send,
    counts_recv,
    site_send,
    site_recv,
):
    g = lax.axis_index("cls")
    me = lax.axis_index("site")
    side = lax.rem(me, SIDES)
    hub = side == SIDES - 1
    hub_site = me + SIDES - 1 - side
    tiles, folds, _, _ = codes.shape
    local = tiles * 8
    taxa = local * groups
    classes, branches = lengths_ref.shape
    halves = folds // groups
    low = LEVELS - TOP
    clades = local >> low
    rows = halves * classes
    f32 = jnp.float32

    copies = []
    small = [
        (freq_hbm, freq_ref),
        (lengths_hbm, lengths_ref),
        (kids_hbm, kids),
        (weights_hbm, weights_ref),
        (counts_hbm, counts),
    ]
    for n, (source, target) in enumerate(small):
        copies.append(pltpu.make_async_copy(source, target, in_sem.at[n]))
        copies[-1].start()
    fetches = []
    for fold in range(folds):
        lanes = pl.ds(fold * LANES, LANES)
        fetches.append(
            pltpu.make_async_copy(codes_hbm.at[:, :, lanes], codes.at[:, fold], code_sem.at[fold])
        )
        fetches[-1].start()

    barrier = pltpu.get_barrier_semaphore()
    others = [(a, b) for a in range(groups) for b in range(site_devices) if a or b]
    for a, b in others:
        pl.semaphore_signal(
            barrier,
            inc=1,
            device_id={"cls": lax.rem(g + a, groups), "site": lax.rem(me + b, site_devices)},
            device_id_type=MESH,
        )

    copies[0].wait()
    freq = [jnp.broadcast_to(freq_ref[:, i : i + 1], (classes, LANES)) for i in range(4)]
    whole_freq = (freq[0] + freq[1]) + (freq[2] + freq[3])
    pi = [own / whole_freq for own in freq]
    beta = 1.0 / (1.0 - ((pi[0] * pi[0] + pi[1] * pi[1]) + (pi[2] * pi[2] + pi[3] * pi[3])))
    width = table.shape[1]
    table[classes:8, :] = jnp.zeros((8 - classes, width), f32)
    for c in range(classes):
        for i in range(4):
            stat[c, i] = jnp.broadcast_to(pi[i][c : c + 1], (8, LANES))
            pick[c, i : i + 1] = pi[i][c : c + 1]
            pick[c, i + 4 : i + 5] = pi[i][c : c + 1]
    copies[1].wait()
    for at in range(0, width, LANES):
        end = min(at + LANES, branches)
        table[0:classes, at:end] = jnp.exp(beta[:, : end - at] * lengths_ref[:, at:end]) - 1.0
    wide_levels = [h for h in range(low) if (local >> h) % LANES == 0]
    tail_start = level_base(taxa, len(wide_levels)) // LANES * LANES
    offset = {}
    total_rows = 0
    for h in range(low):
        count = local >> h
        offset[h] = total_rows
        if h in wide_levels:
            here = pl.ds(pl.multiple_of(level_base(taxa, h) + g * count, LANES), count)
            columns[total_rows : total_rows + count, :] = table[:, here].T
        total_rows += count
    tail[...] = table[:, tail_start:width].T
    per = [(local >> h) // clades for h in range(low + 1)]

    def fill(h, start, count):
        if h in wide_levels:
            column = columns[pl.ds(pl.multiple_of(offset[h] + start, 8), count), :]
        else:
            base = level_base(taxa, h) - tail_start + g * (local >> h)
            column = tail[pl.ds(pl.multiple_of(base + start, 8), count), :]
        target = pl.ds(pl.multiple_of(offset[h] + start, 8), count)
        for c in range(classes):
            grow[c, target, :] = jnp.broadcast_to(column[:, c : c + 1], (count, LANES))

    for h in range(low):
        fill(h, 0, local >> h)
    copies[2].wait()
    for fetch in fetches:
        fetch.wait()
    flat = codes.reshape(local * folds, LANES)

    def child_row(side, level, node):
        return kids[side, taxa - (taxa >> (level - 1)) + node]

    def factor(c, h, node):
        return grow[c, pl.ds(offset[h] + node, 1), :]

    def tip_codes(tip):
        return flat[pl.ds((tip >> 3) * (8 * folds) + (tip & 7), folds, stride=8), :]

    def spread(c, values, scale):
        mean = (values[0] * stat[c, 0] + values[1] * stat[c, 1]) + (
            values[2] * stat[c, 2] + values[3] * stat[c, 3]
        )
        move = scale * mean
        return [value + move for value in values], mean

    span = classes // PIECES

    def step(index, carry):
        p = index // clades
        j = lax.rem(index, clades)
        mine = [span * p + n for n in range(span)]
        for n in range(per[1]):
            node = j * per[1] + n
            left = child_row(0, 1, g * (local >> 1) + node) & (local - 1)
            right = child_row(1, 1, g * (local >> 1) + node) & (local - 1)
            a = tip_codes(left)
            b = tip_codes(right)
            same = jnp.where(a == b, 1.0, 0.0)
            in_a = [a == i for i in range(4)]
            in_b = [b == i for i in range(4)]
            for q, c in enumerate(mine):
                pi_a = look_up(pick[c], a)
                pi_b = look_up(pick[c], b)
                off_a = factor(c, 0, left) * pi_a
                off_b = factor(c, 0, right) * pi_b
                on_b = off_b + same
                mean = off_a * (pi_b + off_b) + pi_a * on_b
                move = factor(c, 1, node) * mean
                at_a = (off_a + 1.0) * on_b + move
                at_b = (off_b + 1.0) * (off_a + same) + move
                rest = off_a * off_b + move
                for i in range(4):
                    pairs[n, 4 * q + i] = jnp.where(
                        in_a[i], at_a, jnp.where(in_b[i], at_b, rest)
                    )
        logs = [None] * span
        for n in range(per[3]):
            node = j * per[3] + n
            seconds = [
                child_row(side, 3, g * (local >> 3) + node) & (per[2] - 1) for side in (0, 1)
            ]
            firsts = [
                [
                    child_row(side, 2, g * (local >> 2) + j * per[2] + second) & (per[1] - 1)
                    for side in (0, 1)
                ]
                for second in seconds
            ]
            for q, c in enumerate(mine):
                both = []
                for second, first in zip(seconds, firsts):
                    values = [
                        pairs[first[0], 4 * q + i] * pairs[first[1], 4 * q + i] for i in range(4)
                    ]
                    both.append(spread(c, values, factor(c, 2, j * per[2] + second))[0])
                values = [x * y for x, y in zip(*both)]
                values, mean = spread(c, values, factor(c, 3, node))
                scale = pl.reciprocal(mean, approx=True)
                logs[q] = jnp.log(scale) if n == 0 else logs[q] + jnp.log(scale)
                for i in range(4):
                    mids[n, 4 * q + i] = values[i] * scale
        fourths = [
            [child_row(side, 5, g * (local >> 5) + j * per[5] + n) & (per[4] - 1) for side in (0, 1)]
            for n in range(per[5])
        ]
        thirds = [
            [
                [
                    child_row(side, 4, g * (local >> 4) + j * per[4] + fourth) & (per[3] - 1)
                    for side in (0, 1)
                ]
                for fourth in pair
            ]
            for pair in fourths
        ]
        for q, c in enumerate(mine):
            top = []
            for n in range(per[5]):
                both = []
                for fourth, third in zip(fourths[n], thirds[n]):
                    values = [
                        mids[third[0], 4 * q + i] * mids[third[1], 4 * q + i] for i in range(4)
                    ]
                    both.append(spread(c, values, factor(c, 4, j * per[4] + fourth))[0])
                values = [x * y for x, y in zip(*both)]
                top.append(spread(c, values, factor(c, 5, j * per[5] + n))[0])
            values = [x * y for x, y in zip(*top)]
            inverse = 1.0 / values[3]
            for i in range(3):
                ratio = values[i] * inverse
                for block in range(groups):
                    sent[block, p, j, i, halves * q : halves * (q + 1), :] = ratio[
                        halves * block : halves * (block + 1)
                    ]
            before = jnp.where(j == 0, 0.0, scale_sum[q])
            total = before + (jnp.log(values[3]) - logs[q])
            scale_sum[q] = total
            for block in range(groups):
                sent_scale[block, p, halves * q : halves * (q + 1), :] = total[
                    halves * block : halves * (block + 1)
                ]

        @pl.when(index == 0)
        def _():
            pl.semaphore_wait(barrier, len(others))

        def to_hub(source, target, slot, send, recv):
            copy = pltpu.make_async_remote_copy(
                src_ref=source,
                dst_ref=target,
                send_sem=send,
                recv_sem=recv.at[side],
                device_id={"cls": partner(slot), "site": hub_site},
                device_id_type=MESH,
            )
            if slot:
                copy.start()
            else:
                pl.when(jnp.logical_not(hub))(copy.start)

        for slot in order:
            to_hub(
                sent.at[partner(slot), p, j], got.at[slot, p, j, :, side], slot, send_sem, recv_sem
            )

        @pl.when(j == clades - 1)
        def _():
            for slot in order:
                to_hub(
                    sent_scale.at[partner(slot), p],
                    got_scale.at[slot, p, side],
                    slot,
                    scale_send,
                    scale_recv,
                )

        return carry

    xor = groups & (groups - 1) == 0
    order = ([2, 3, 1] if groups == 4 else list(range(1, groups))) + [0]

    def partner(slot):
        return g ^ slot if xor else lax.rem(g + slot, groups)

    def slot_of(source):
        return g ^ source if xor else lax.rem(source + groups - g, groups)

    lax.fori_loop(0, PIECES * clades, step, 0)
    for p in range(PIECES):
        for j in range(clades):
            for i in range(3):
                got[0, p, j, i, SIDES - 1] = sent[g, p, j, i]
        got_scale[0, p, SIDES - 1] = sent_scale[g, p]
    for copy in copies[3:]:
        copy.wait()
    counts_copy = pltpu.make_async_remote_copy(
        src_ref=counts,
        dst_ref=counts_got,
        send_sem=counts_send,
        recv_sem=counts_recv,
        device_id={"site": hub_site},
        device_id_type=MESH,
    )
    pl.when(jnp.logical_not(hub))(counts_copy.start)
    first_up = level_base(taxa, low)
    window = first_up // LANES * LANES
    r8 = jnp.concatenate([table[n // halves : n // halves + 1, window:branches] for n in range(rows)], axis=0)
    for j in range(branches - first_up):
        at = first_up - window + j
        grow_up[j] = jnp.broadcast_to(r8[:, at : at + 1], (rows, LANES))
    drift = beta[:, 0:1] * jnp.sum(lengths_ref[...], axis=1, keepdims=True)
    pis8 = [
        jnp.concatenate([stat[n // halves, i, 0:1] for n in range(rows)], axis=0) for i in range(4)
    ]
    spot = lax.broadcasted_iota(jnp.int32, (classes, classes), 0)
    spot = spot == lax.broadcasted_iota(jnp.int32, (classes, classes), 1)
    weights = jnp.sum(jnp.where(spot, weights_ref[...], 0.0), axis=1, keepdims=True)
    log_weight = jnp.log(weights / jnp.sum(weights, axis=0, keepdims=True))
    bias = log_weight - drift
    bias = jnp.concatenate([bias[n // halves : n // halves + 1] for n in range(rows)], axis=0)
    def over_halves(x):
        return functools.reduce(
            jnp.add, [x[d, h : h + 1] for d in range(SIDES) for h in range(halves)]
        )

    sources = groups * (site_devices // SIDES)

    @pl.when(hub)
    def _():
        near = got.at[:, :, :, :, 0]
        far = got.at[pl.ds(1, groups - 1), :, :, :, 1]
        pltpu.make_async_copy(near, near, recv_sem.at[0]).wait()
        pltpu.make_async_copy(far, far, recv_sem.at[1]).wait()
        near = got_scale.at[:, :, 0]
        far = got_scale.at[pl.ds(1, groups - 1), :, 1]
        pltpu.make_async_copy(near, near, scale_recv.at[0]).wait()
        pltpu.make_async_copy(far, far, scale_recv.at[1]).wait()
        pltpu.make_async_copy(counts_got, counts_got, counts_recv).wait()
        quarter = pl.ds(g * halves, halves)
        seen_at = jnp.stack([counts_got[quarter, :], counts[quarter, :]]).astype(f32)

        def whole(*parts):
            return parts[0] if len(parts) == 1 else jnp.concatenate(parts, axis=0)

        scales = functools.reduce(jnp.add, [whole(*[got_scale[k, p] for p in range(PIECES)]) for k in range(groups)])

        def child(tree_level, ident):
            if tree_level == low:
                place = (ident - first_up) & (2**TOP - 1)
                k = slot_of(place // clades)
                j = lax.rem(place, clades)
                values = [whole(*[got[k, p, j, i] for p in range(PIECES)]) for i in range(3)]
                values.append(jnp.ones((SIDES, rows, LANES), f32))
            else:
                at = jnp.clip(ident - level_base(taxa, low + 1), 0, 2**TOP - 1)
                values = [upper[at, i] for i in range(4)]
            mean = (values[0] * pis8[0] + values[1] * pis8[1]) + (
                values[2] * pis8[2] + values[3] * pis8[3]
            )
            move = grow_up[jnp.clip(ident - first_up, 0, branches - first_up - 1)] * mean
            return [value + move for value in values]

        place = 0
        for tree_level in range(low, LEVELS):
            count = taxa >> (tree_level + 1)
            first = taxa - (taxa >> tree_level)
            for n in range(count):
                left = child(tree_level, kids[0, first + n])
                right = child(tree_level, kids[1, first + n])
                values = [a * b for a, b in zip(left, right)]
                largest = jnp.maximum(
                    jnp.maximum(values[0], values[1]), jnp.maximum(values[2], values[3])
                )
                scale = pl.reciprocal(largest, approx=True)
                scales = scales - jnp.log(scale)
                values = [value * scale for value in values]
                if tree_level < LEVELS - 1:
                    for i in range(4):
                        upper[place, i] = values[i]
                    place += 1
        end = (values[0] * pis8[0] + values[1] * pis8[1]) + (
            values[2] * pis8[2] + values[3] * pis8[3]
        )
        shifted = scales + jnp.log(end) + bias
        each = [shifted[:, halves * c : halves * (c + 1)] for c in range(classes)]
        top = functools.reduce(jnp.maximum, each)
        total = top + jnp.log(functools.reduce(jnp.add, [jnp.exp(a - top) for a in each]))
        site_sent[...] = total[0] / taxa

        loglik = over_halves(seen_at * total)
        seen = over_halves(seen_at)
        sums = [over_halves(seen_at * jnp.exp(a - total)) for a in each] + [loglik, seen]
        size = len(sums)
        sums = jnp.sum(jnp.concatenate(sums, axis=0), axis=1, keepdims=True)
        lane = lax.broadcasted_iota(jnp.int32, (size, LANES), 1)
        spot = lane == lax.broadcasted_iota(jnp.int32, (size, LANES), 0)
        part[...] = jnp.sum(jnp.where(spot, sums, 0.0), axis=0, keepdims=True)
        own = g * (site_devices // SIDES) + me // SIDES
        site_copy = pltpu.make_async_remote_copy(
            src_ref=site_sent,
            dst_ref=site_got,
            send_sem=site_send,
            recv_sem=site_recv,
            device_id={"site": me + 1 - SIDES},
            device_id_type=MESH,
        )
        site_copy.start()
        for a, b in reversed(others):
            pltpu.make_async_remote_copy(
                src_ref=part,
                dst_ref=part_got.at[own],
                send_sem=part_send,
                recv_sem=part_recv,
                device_id={"cls": lax.rem(g + a, groups), "site": lax.rem(me + b, site_devices)},
                device_id_type=MESH,
            ).start()
        part_got[own] = part[...]
        result[0:halves, :] = total[SIDES - 1] / taxa
        rest = part_got.at[pl.ds(0, sources - 1)]
        pltpu.make_async_copy(rest, rest, part_recv).wait()
        sends = part_sink.at[pl.ds(0, len(others))]
        pltpu.make_async_copy(sends, sends, part_send).wait()
        site_copy.wait_send()
        done = sent.at[pl.ds(0, groups - 1)]
        pltpu.make_async_copy(done, done, send_sem).wait()
        done = sent_scale.at[pl.ds(0, groups - 1)]
        pltpu.make_async_copy(done, done, scale_send).wait()

    @pl.when(jnp.logical_not(hub))
    def _():
        counts_copy.wait_send()
        pltpu.make_async_copy(sent, sent, send_sem).wait()
        pltpu.make_async_copy(sent_scale, sent_scale, scale_send).wait()
        pltpu.make_async_copy(site_got, site_got, site_recv).wait()
        result[0:halves, :] = site_got[...]
        pltpu.make_async_copy(part_got, part_got, part_recv).wait()

    line = [part_got[d] for d in range(sources)]
    while len(line) > 1:
        line = [jnp.add(*line[d : d + 2]) if d + 1 < len(line) else line[d] for d in range(0, len(line), 2)]
    lane = lax.broadcasted_iota(jnp.int32, (3, LANES), 1)
    row = lax.broadcasted_iota(jnp.int32, (3, LANES), 0)
    spot = lane == jnp.where(row == 0, g, classes - 1 + row)
    line = jnp.sum(jnp.where(spot, line[0], 0.0), axis=1, keepdims=True)
    all_count = line[2:3]
    mean = line[1:2] / (all_count * taxa)
    share = line[0:1] / all_count
    result[halves : halves + 1, :] = jnp.broadcast_to(share, (1, LANES))
    result[halves + 1 : halves + 2, :] = jnp.broadcast_to(mean, (1, LANES))


def finish(result, site_out, weight_out, mean_out):
    halves = result.shape[0] - 2
    for half in range(halves):
        site_out[0:1, half * LANES : (half + 1) * LANES] = result[half : half + 1, :]
    weight_out[...] = result[halves : halves + 1, 0:1]
    mean_out[...] = result[halves + 1 : halves + 2, 0:1]


def solution(mesh):
    groups = mesh.shape["cls"]
    site_devices = mesh.shape["site"]

    def per_device(tip_codes, counts, children, lengths, frequencies, weights):
        local, sites = tip_codes.shape
        taxa = local * groups
        classes, branches = lengths.shape
        quarter = sites // groups
        halves = quarter // LANES
        rows = halves * classes
        low = LEVELS - TOP
        clades = local >> low
        low_rows = sum(local >> h for h in range(low))
        table_width = -(-branches // LANES) * LANES
        wide_levels = [h for h in range(low) if (local >> h) % LANES == 0]
        tail_start = level_base(taxa, len(wide_levels)) // LANES * LANES
        folds = sites // LANES
        up_count = branches - level_base(taxa, low)
        kids = children.T
        vmem = pl.BlockSpec(memory_space=pltpu.VMEM)
        hbm = pl.BlockSpec(memory_space=pltpu.HBM)
        f32 = jnp.float32
        result = pl.pallas_call(
            functools.partial(kernel, groups, site_devices),
            out_shape=jax.ShapeDtypeStruct((halves + 2, LANES), f32),
            in_specs=[hbm] * 6,
            out_specs=vmem,
            scratch_shapes=[
                pltpu.VMEM((local // 8, folds, 8, LANES), jnp.int32),
                pltpu.VMEM((folds, LANES), jnp.int32),
                pltpu.SMEM(kids.shape, jnp.int32),
                pltpu.VMEM(lengths.shape, f32),
                pltpu.VMEM(frequencies.shape, f32),
                pltpu.VMEM((1, classes), f32),
                pltpu.VMEM((8, table_width), f32),
                pltpu.VMEM((sum(local >> h for h in wide_levels), 8), f32),
                pltpu.VMEM((table_width - tail_start, 8), f32),
                pltpu.VMEM((classes, low_rows, LANES), f32),
                pltpu.VMEM((up_count, rows, LANES), f32),
                pltpu.VMEM((classes, 4, 8, LANES), f32),
                pltpu.VMEM((classes, 8, LANES), f32),
                pltpu.VMEM(((local >> 1) // clades, 4 * classes // PIECES, folds, LANES), f32),
                pltpu.VMEM(((local >> 3) // clades, 4 * classes // PIECES, folds, LANES), f32),
                pltpu.VMEM((classes // PIECES, folds, LANES), f32),
                pltpu.VMEM((groups, PIECES, clades, 3, rows // PIECES, LANES), f32),
                pltpu.VMEM((groups, PIECES, clades, 3, SIDES, rows // PIECES, LANES), f32),
                pltpu.VMEM((groups, PIECES, rows // PIECES, LANES), f32),
                pltpu.VMEM((groups, PIECES, SIDES, rows // PIECES, LANES), f32),
                pltpu.VMEM((2 ** TOP, 4, SIDES, rows, LANES), f32),
                pltpu.VMEM((folds, LANES), jnp.int32),
                pltpu.VMEM((halves, LANES), f32),
                pltpu.VMEM((halves, LANES), f32),
                pltpu.VMEM((1, LANES), f32),
                pltpu.VMEM((groups * site_devices // SIDES, 1, LANES), f32),
                pltpu.VMEM((groups * site_devices, 1, LANES), f32),
                pltpu.SemaphoreType.DMA((5,)),
                pltpu.SemaphoreType.DMA((folds,)),
                pltpu.SemaphoreType.DMA,
                pltpu.SemaphoreType.DMA((SIDES,)),
                pltpu.SemaphoreType.DMA,
                pltpu.SemaphoreType.DMA((SIDES,)),
                pltpu.SemaphoreType.DMA,
                pltpu.SemaphoreType.DMA,
                pltpu.SemaphoreType.DMA,
                pltpu.SemaphoreType.DMA,
                pltpu.SemaphoreType.DMA,
                pltpu.SemaphoreType.DMA,
            ],
            compiler_params=pltpu.CompilerParams(collective_id=0, has_side_effects=True, vmem_limit_bytes=32 << 20),
        )(
            *(
                pltpu.with_memory_space_constraint(operand, pltpu.HBM)
                for operand in (
                    tip_codes.reshape(local // 8, 8, sites),
                    counts.reshape(folds, LANES),
                    kids,
                    lengths,
                    frequencies,
                    weights.reshape(1, classes),
                )
            )
        )
        site_loglik, new_weights, mean_loglik = pl.pallas_call(
            finish,
            out_shape=(
                jax.ShapeDtypeStruct((1, quarter), f32),
                jax.ShapeDtypeStruct((1, 1), f32),
                jax.ShapeDtypeStruct((1, 1), f32),
            ),
            in_specs=[vmem],
            out_specs=(vmem, vmem, vmem),
            compiler_params=pltpu.CompilerParams(vmem_limit_bytes=1 << 20),
        )(result)
        return site_loglik, new_weights.reshape(1), mean_loglik.reshape(())

    return jax.shard_map(
        per_device,
        mesh=mesh,
        in_specs=(P("cls", "site"), P("site"), P(), P(), P(), P()),
        out_specs=(P("cls", "site"), P("cls"), P()),
        check_vma=False,
    )
```
